32 devices in a mesh: section: 4 (over z), col: 8 (over y, x, core).
Axes of the slice: x: 2, y: 2, z: 4, core: 2. Of those that a mesh axis runs over, the one named last changes fastest.
Arguments:
- tiles: bfloat16 [256, 12, 128, 128], P('col', None, 'section'), may hold values from 0.0099487305 to 1
- offsets: int32 [256, 12], replicated, may hold values from -6 to 6, as said below
- counts: int32 [256], replicated, may hold values from 1 to 12
- ranks: int32 [256, 25, 128, 128], P('col', None, 'section'), may hold values from 0 to 3199, as said below
Outputs:
- pruned: bfloat16 [256, 25, 128, 128], P('col', None, 'section')
The draws below stay inside these ranges and needn't reach their ends.
Inputs may be any that keep to these rules, and one draw needn't show every extreme that they name: Within each panel the 12 offsets are distinct, each from -6 to 6. For every panel j and column c, ranks[j, :, c, :] holds each of 0 .. 3199 once.
All inputs are finite; a program needn't handle non-finite values.
Results may differ from the reference program's by a relative error of at most 0.001.
Values may be sent and summed in bfloat16 or wider, within the bound.
A program may use at most 128 MiB of HBM per device.

```python
import math
import jax
import jax.numpy as jnp
from jax import lax

TILE = 128
KB = 12
W = 6
TOPK = 256
NB = 256
OB = 25


def draw_offsets(key, part):
    keys = jax.random.split(key, NB)
    perms = jax.vmap(lambda single: jax.random.permutation(single, 2 * W + 1))(keys)
    return (perms[:, :KB] - W).astype(jnp.int32)


def draw_ranks(key, part):
    keys = jax.random.split(key, NB * TILE)
    perms = jax.vmap(lambda single: jax.random.permutation(single, OB * TILE))(keys)
    return perms.reshape(NB, TILE, OB, TILE).transpose(0, 2, 1, 3).astype(jnp.int32)


def place_ends(array, rng, least, largest):
    longest = array.shape.index(max(array.shape))
    spots = []
    for shift in (0, 1):
        where = [jax.random.randint(jax.random.fold_in(rng, axis), (), 0, length) for axis, length in enumerate(array.shape)]
        where[longest] = (where[longest] + shift) % array.shape[longest]
        spots.append(tuple(where))
    return array.at[spots[0]].set(least).at[spots[1]].set(largest)


def levels(stream_key, shape, pieces, least, high):
    def one(position, shards_of):
        heights = jax.random.uniform(jax.random.fold_in(jax.random.fold_in(stream_key, 6), position), (shards_of,), jnp.float32, least / len(pieces), high / len(pieces))
        return jnp.repeat(jnp.exp(heights), shape[position] // shards_of).reshape((-1,) + (1,) * (len(shape) - position - 1))

    factor_of = one(*pieces[0])
    for cut in pieces[1:]:
        factor_of = factor_of * one(*cut)
    return factor_of


def setup_inputs(seed: int = 0) -> dict:
    key_of = jax.random.split(jax.random.key(seed), 5)
    tiles = jnp.clip(jnp.exp(math.log(1.0) - 4.61031033 * jax.random.uniform(key_of[0], (NB, KB, TILE, TILE), jnp.float32) ** levels(key_of[0], (NB, KB, TILE, TILE), ((0, 8), (2, 4)), -0.2, 0.2)), 0.0099487305, 1.0).astype(jnp.bfloat16)
    offsets = draw_offsets(jax.random.fold_in(key_of[4], 71), 0)
    counts = place_ends(jax.random.randint(key_of[2], (NB,), 1, KB + 1), jax.random.fold_in(key_of[2], 1), 1, KB).astype(jnp.int32)
    ranks = draw_ranks(jax.random.fold_in(key_of[4], 71), 0)
    return {"tiles": tiles, "offsets": offsets, "counts": counts, "ranks": ranks}


def reference(tiles, offsets, counts, ranks):
    total = tiles.shape[0]
    slots = tiles.shape[1]
    bands = 4 * W + 1
    padded = jnp.pad(tiles, ((W, W), (0, 0), (0, 0), (0, 0)))
    pad_off = jnp.pad(offsets, ((W, W), (0, 0)))
    pad_cnt = jnp.pad(counts, ((W, W),))
    slot_ids = jnp.arange(slots, dtype=jnp.int32)

    def one_panel(panel):
        own = lax.dynamic_index_in_dim(tiles, panel, 0, False).astype(jnp.float32)
        own_off = lax.dynamic_index_in_dim(offsets, panel, 0, False)
        own_cnt = lax.dynamic_index_in_dim(counts, panel, 0, False)
        where_at = (panel + W + own_off).astype(jnp.int32)
        firsts = padded[where_at].astype(jnp.float32)
        first_off = pad_off[where_at]
        first_cnt = pad_cnt[where_at]
        row_own = panel + own_off
        ok_own = (slot_ids < own_cnt) & (row_own >= 0) & (row_own < total)
        row_first = row_own[:, None] + first_off
        ok_first = (slot_ids[None, :] < first_cnt[:, None]) & (row_first >= 0) & (row_first < total)
        weight = (ok_own[:, None] & ok_first).astype(jnp.float32)
        target = own_off[:, None] + first_off + 2 * W
        place = (jnp.arange(bands, dtype=jnp.int32)[:, None, None] == target[None]).astype(jnp.float32) * weight[None]
        products = jnp.einsum('kcx,klxr->klcr', own, firsts, precision=lax.Precision.HIGHEST)
        expanded = jnp.einsum('okl,klcr->ocr', place, products, precision=lax.Precision.HIGHEST)
        keep = lax.dynamic_index_in_dim(ranks, panel, 0, False) < TOPK
        squared = jnp.where(keep, expanded * expanded, jnp.float32(0.0))
        totals = jnp.sum(squared, axis=(0, 2), keepdims=True)
        return (TOPK * squared / (totals + 1e-6)).astype(jnp.bfloat16)

    return lax.map(one_panel, jnp.arange(total, dtype=jnp.int32))
```

```python
import functools

import jax
import jax.numpy as jnp
from jax import lax
from jax.experimental import pallas as pl
from jax.experimental.pallas import tpu as pltpu
from jax.sharding import PartitionSpec as P

W = 6
TOPK = 256
HALF = 6


def panel_kernel(
    bands, slots, parts, panel_of,
    own_start, own_count, own_off, band_start, band_count, band_off,
    *refs,
):
    n_parts = len(parts)
    sources = refs[:n_parts]
    own_ref, ranks_ref = refs[n_parts], refs[n_parts + 1]
    out_ref, band, acc, sems = refs[-4:]
    step = pl.program_id(0)

    @pl.when(step == 0)
    def _():
        copies = [
            pltpu.make_async_copy(src, band.at[pl.ds(at, src.shape[0])], sems.at[i])
            for i, (src, at) in enumerate(zip(sources, parts))
        ]
        for copy in copies:
            copy.start()
        for copy in copies:
            copy.wait()

    panel = panel_of(step)
    acc[...] = jnp.zeros_like(acc)
    first = own_start[panel]

    def one_slot(q, carry):
        off = own_off[q]
        source = panel + W + off
        start = band_start[source]
        count = band_count[source]
        lhs = own_ref[q]

        def group(base):
            for i in range(base, min(base + HALF, slots)):
                product = jnp.dot(lhs, band[start + i], preferred_element_type=jnp.float32)
                where = jnp.where(i < count, off + band_off[start + i] + 2 * W, bands)
                acc[where] += product

        group(0)
        for base in range(HALF, slots, HALF):
            pl.when(count > base)(functools.partial(group, base))
        return carry

    lax.fori_loop(first, first + own_count[panel], one_slot, 0)

    total = jnp.zeros(acc.shape[1:], jnp.float32)
    for o in range(bands):
        value = acc[o]
        squared = jnp.where(ranks_ref[0, o] < TOPK, value * value, 0.0)
        acc[o] = squared
        total = total + squared
    totals = jnp.sum(total, axis=1, keepdims=True) + 1e-06
    scale = jnp.broadcast_to(TOPK / totals, total.shape)
    for o in range(bands):
        out_ref[0, o] = (acc[o] * scale).astype(out_ref.dtype)


def run_panels(scalars, sources, parts, size, own, ranks, steps, panel_of, previous):
    panels, bands, columns, rows = ranks.shape
    slots = scalars[-1]
    tables = scalars[:-1]
    block = (1, bands, columns, rows)
    panel_block = pl.BlockSpec(block, lambda i, *_: (panel_of(i), 0, 0, 0))
    operands = [*sources, own, ranks]
    specs = [pl.BlockSpec(memory_space=pl.ANY)] * len(sources)
    specs += [pl.BlockSpec(own.shape, lambda i, *_: (0, 0, 0)), panel_block]
    aliases = {}
    if previous is not None:
        aliases = {len(tables) + len(operands): 0}
        operands.append(previous)
        specs.append(pl.BlockSpec(memory_space=pl.ANY))
    return pl.pallas_call(
        functools.partial(panel_kernel, bands, slots, parts, panel_of),
        grid_spec=pltpu.PrefetchScalarGridSpec(
            num_scalar_prefetch=len(tables),
            grid=(steps,),
            in_specs=specs,
            out_specs=panel_block,
            scratch_shapes=[
                pltpu.VMEM((size, rows, rows), jnp.bfloat16),
                pltpu.VMEM((bands + 1, columns, rows), jnp.float32),
                pltpu.SemaphoreType.DMA((len(sources),)),
            ],
        ),
        out_shape=jax.ShapeDtypeStruct(ranks.shape, jnp.bfloat16),
        input_output_aliases=aliases,
        compiler_params=pltpu.CompilerParams(
            dimension_semantics=("arbitrary",), vmem_limit_bytes=56 * 2**20
        ),
        cost_estimate=pl.CostEstimate(
            flops=steps * 40 * 10**6, bytes_accessed=steps * 2 * 10**6, transcendentals=0
        ),
    )(*tables, *operands)


def shards(tiles, offsets, counts, ranks):
    panels, slots, columns, rows = tiles.shape
    total = offsets.shape[0]
    groups = lax.axis_size("col")
    me = lax.axis_index("col")
    full = panels * slots
    halo = W * slots

    slot_ids = jnp.arange(slots, dtype=jnp.int32)[None]
    row_of = jnp.arange(total, dtype=jnp.int32)[:, None] + offsets
    valid = (slot_ids < counts[:, None]) & (row_of >= 0) & (row_of < total)
    valid = valid.reshape(groups, full)
    needed = jnp.max(jnp.sum(valid.astype(jnp.int32), axis=1))

    def three(array):
        padded = jnp.pad(array, ((1, 1), (0, 0)))
        return lax.dynamic_slice_in_dim(padded, me, 3, 0)

    near_valid = three(valid.astype(jnp.int32))
    near_off = three(offsets.reshape(groups, full))
    ids = jnp.arange(full, dtype=jnp.int32)
    position = jnp.sum(
        jnp.where(ids[None, None, :] < ids[None, :, None], near_valid[:, None, :], 0), axis=2
    )
    packed = jnp.where(near_valid > 0, position, -1)
    match = packed[:, None, :] == ids[None, :, None]
    packed_off = jnp.sum(jnp.where(match, near_off[:, None, :], 0), axis=2)
    packed_id = jnp.sum(jnp.where(match[1], ids[None, :], 0), axis=1)
    panel_start = position.reshape(3, panels, slots)[:, :, 0]
    panel_count = jnp.sum(near_valid.reshape(3, panels, slots), axis=2)
    last_start = jnp.sum(near_valid, axis=1) - halo

    flat = tiles.reshape(full, columns, rows)
    up = [(i, i + 1) for i in range(groups - 1)]
    down = [(i + 1, i) for i in range(groups - 1)]

    def at_capacity(capacity):
        def run():
            own = flat[packed_id[:capacity]]
            gathered = lax.all_gather(own, "section", axis=1, tiled=True)
            starts = jnp.clip(last_start, 0, capacity - halo)
            last = lax.dynamic_slice_in_dim(gathered, starts[1], halo, 0)
            before = lax.ppermute(last, "col", up)
            after = lax.ppermute(gathered[:halo], "col", down)

            band_start = jnp.concatenate([
                panel_start[0, panels - W:] - starts[0],
                panel_start[1] + halo,
                panel_start[2, :W] + halo + capacity,
            ])
            band_count = jnp.concatenate(
                [panel_count[0, panels - W:], panel_count[1], panel_count[2, :W]]
            )
            band_off = jnp.concatenate([
                lax.dynamic_slice_in_dim(packed_off[0], starts[0], halo, 0),
                packed_off[1, :capacity],
                packed_off[2, :halo],
                jnp.zeros((slots,), jnp.int32),
            ])
            scalars = (
                panel_start[1], panel_count[1], packed_off[1],
                band_start, band_count, band_off, slots,
            )
            size = capacity + 2 * halo + slots
            inner = run_panels(
                scalars, [gathered], [halo], size, own, ranks,
                panels - 2 * W, lambda i: i + W, None,
            )
            return run_panels(
                scalars, [before, gathered, after], [0, halo, halo + capacity], size, own, ranks,
                2 * W, lambda i: jnp.where(i < W, i, i + panels - 2 * W), inner,
            )
        return run

    levels = sorted({max(halo, full * part // 24) for part in (14, 15, 16, 18, 24)})
    which = sum((needed > level).astype(jnp.int32) for level in levels[:-1])
    return lax.switch(which, [at_capacity(level) for level in levels])


def solution(mesh):
    placed = (P("col", None, "section", None), P(), P(), P("col", None, "section", None))
    return jax.shard_map(
        shards,
        mesh=mesh,
        in_specs=placed,
        out_specs=P("col", None, "section", None),
        check_vma=False,
    )
```

```python
import functools

import jax
import jax.numpy as jnp
from jax import lax
from jax.experimental import pallas as pl
from jax.experimental.pallas import tpu as pltpu
from jax.sharding import PartitionSpec as P

W = 6
TOPK = 256
HALF = 6


def panel_kernel(
    bands, slots, parts, early, limit,
    own_start, own_count, own_off, own_id, band_start, band_count, band_off,
    *refs,
):
    n_parts = len(parts)
    sources = refs[:n_parts]
    own_ref = refs[n_parts]
    out_ref, band, acc, sems = refs[-4:]
    step = pl.program_id(0)

    @pl.when(step == 0)
    def _():
        copies = [
            pltpu.make_async_copy(src, band.at[pl.ds(at, src.shape[0])], sems.at[i])
            for i, (src, at) in enumerate(zip(sources, parts))
        ]
        for copy in copies:
            copy.start()
        for copy in copies:
            copy.wait()

    panel = step
    panels = pl.num_programs(0)
    if early:
        acc[...] = jnp.zeros_like(acc)
    else:
        ranks_ref, sums_ref = refs[n_parts + 1], refs[n_parts + 2]
        acc[:bands] = sums_ref[0]
    first = own_start[panel]

    def one_slot(q, carry):
        off = own_off[q]
        source = panel + W + off
        start = band_start[source]
        count = band_count[source]
        lhs = own_ref[own_id[q]]
        inside = (source >= W) & (source < panels + W) & (start + count <= limit)
        mine = inside if early else jnp.logical_not(inside)

        def group(base):
            for i in range(base, min(base + HALF, slots)):
                product = jnp.dot(lhs, band[start + i], preferred_element_type=jnp.float32)
                where = jnp.where(i < count, off + band_off[start + i] + 2 * W, bands)
                acc[where] += product

        for base in range(0, slots, HALF):
            pl.when(mine & (count > base))(functools.partial(group, base))
        return carry

    lax.fori_loop(first, first + own_count[panel], one_slot, 0)

    if early:
        out_ref[0] = acc[:bands]
        return
    total = jnp.zeros(acc.shape[1:], jnp.float32)
    for o in range(bands):
        value = acc[o]
        squared = jnp.where(ranks_ref[0, o] < TOPK, value * value, 0.0)
        acc[o] = squared
        total = total + squared
    totals = jnp.sum(total, axis=1, keepdims=True) + 1e-06
    scale = jnp.broadcast_to(TOPK / totals, total.shape)
    for o in range(bands):
        out_ref[0, o] = (acc[o] * scale).astype(out_ref.dtype)


def run_panels(tables, slots, sources, parts, limit, size, own, ranks, sums):
    panels, bands, columns, rows = ranks.shape
    early = sums is None
    panel_block = pl.BlockSpec((1, bands, columns, rows), lambda i, *_: (i, 0, 0, 0))
    operands = [*sources, own]
    specs = [pl.BlockSpec(memory_space=pl.ANY)] * len(sources)
    specs += [pl.BlockSpec(own.shape, lambda i, *_: (0, 0, 0))]
    if not early:
        operands += [ranks, sums]
        specs += [panel_block, panel_block]
    kind = jnp.float32 if early else jnp.bfloat16
    return pl.pallas_call(
        functools.partial(panel_kernel, bands, slots, parts, early, limit),
        grid_spec=pltpu.PrefetchScalarGridSpec(
            num_scalar_prefetch=len(tables),
            grid=(panels,),
            in_specs=specs,
            out_specs=panel_block,
            scratch_shapes=[
                pltpu.VMEM((size, rows, rows), jnp.bfloat16),
                pltpu.VMEM((bands + 1, columns, rows), jnp.float32),
                pltpu.SemaphoreType.DMA((len(sources),)),
            ],
        ),
        out_shape=jax.ShapeDtypeStruct(ranks.shape, kind),
        compiler_params=pltpu.CompilerParams(
            dimension_semantics=("arbitrary",), vmem_limit_bytes=56 * 2**20
        ),
        cost_estimate=pl.CostEstimate(
            flops=panels * 10**9, bytes_accessed=panels * 3 * 10**6, transcendentals=0
        ),
    )(*tables, *operands)


def shards(tiles, offsets, counts, ranks):
    panels, slots, columns, rows = tiles.shape
    total = offsets.shape[0]
    groups = lax.axis_size("col")
    me = lax.axis_index("col")
    full = panels * slots
    halo = W * slots

    slot_ids = jnp.arange(slots, dtype=jnp.int32)[None]
    row_of = jnp.arange(total, dtype=jnp.int32)[:, None] + offsets
    valid = (slot_ids < counts[:, None]) & (row_of >= 0) & (row_of < total)
    valid = valid.reshape(groups, full)
    needed = jnp.max(jnp.sum(valid.astype(jnp.int32), axis=1))

    def three(array):
        padded = jnp.pad(array, ((1, 1), (0, 0)))
        return lax.dynamic_slice_in_dim(padded, me, 3, 0)

    near_valid = three(valid.astype(jnp.int32))
    near_off = three(offsets.reshape(groups, full))
    ids = jnp.arange(full, dtype=jnp.int32)
    panel = ids // slots
    inner = (panel >= W) & (panel < panels - W)
    key = ids + jnp.where(inner, full, 0)
    position = jnp.sum(
        jnp.where(key[None, None, :] < key[None, :, None], near_valid[:, None, :], 0), axis=2
    )
    packed = jnp.where(near_valid > 0, position, -1)
    match = packed[:, None, :] == ids[None, :, None]
    packed_off = jnp.sum(jnp.where(match, near_off[:, None, :], 0), axis=2)
    packed_id = jnp.sum(jnp.where(match[1], ids[None, :], 0), axis=1)
    panel_start = position.reshape(3, panels, slots)[:, :, 0]
    panel_count = jnp.sum(near_valid.reshape(3, panels, slots), axis=2)
    starts = jnp.sum(panel_count[:, :W], axis=1)

    flat = tiles.reshape(full, columns, rows)
    up = [(i, i + 1) for i in range(groups - 1)]
    down = [(i + 1, i) for i in range(groups - 1)]

    def at_capacity(capacity):
        cut = max(2 * halo, min(capacity - slots, capacity * 2 // 3))

        def run():
            early = lax.all_gather(flat[packed_id[:cut]], "section", axis=1, tiled=True)
            late = lax.all_gather(flat[packed_id[cut:capacity]], "section", axis=1, tiled=True)
            last = lax.dynamic_slice_in_dim(early, starts[1], halo, 0)
            before = lax.ppermute(last, "col", up)
            after = lax.ppermute(early[:halo], "col", down)

            band_start = jnp.concatenate([
                panel_start[0, panels - W:] - starts[0],
                panel_start[1] + halo,
                panel_start[2, :W] + halo + capacity,
            ])
            band_count = jnp.concatenate(
                [panel_count[0, panels - W:], panel_count[1], panel_count[2, :W]]
            )
            band_off = jnp.concatenate([
                lax.dynamic_slice_in_dim(packed_off[0], starts[0], halo, 0),
                packed_off[1, :capacity],
                packed_off[2, :halo],
                jnp.zeros((slots,), jnp.int32),
            ])
            tables = (
                panel_start[1], panel_count[1], packed_off[1], packed_id,
                band_start, band_count, band_off,
            )
            size = capacity + 2 * halo + slots
            limit = halo + cut
            sums = run_panels(
                tables, slots, [early], [halo], limit, size, flat, ranks, None
            )
            return run_panels(
                tables, slots, [before, early, late, after],
                [0, halo, limit, halo + capacity], limit, size, flat, ranks, sums,
            )
        return run

    levels = sorted({max(2 * halo + slots, full * part // 48) for part in (28, 29, 30, 31, 33, 36, 48)})
    which = sum((needed > level).astype(jnp.int32) for level in levels[:-1])
    return lax.switch(which, [at_capacity(level) for level in levels])


def solution(mesh):
    placed = (P("col", None, "section", None), P(), P(), P("col", None, "section", None))
    return jax.shard_map(
        shards,
        mesh=mesh,
        in_specs=placed,
        out_specs=P("col", None, "section", None),
        check_vma=False,
    )
```
